32 devices in a mesh: replica: 8 (over z, x), shard: 4 (over y, core).
Axes of the slice: x: 2, y: 2, z: 4, core: 2. Of those that a mesh axis runs over, the one named last changes fastest.
Arguments:
- deltas: bfloat16 [8, 2048, 8192], P('replica', 'shard')
- master: float32 [2048, 8192], P('shard', 'replica'), may hold values from -6 to 6
- momentum: float32 [2048, 8192], P('shard', 'replica'), may hold values from -6 to 6
- block_owner: int32 [8, 1], replicated, may hold values from 0 to 3; in each aligned block of 8 rows (0 to 7, 8 to 15, ...) at most 4 rows name the same one
Outputs:
- master_out: float32 [2048, 8192], P('shard', 'replica')
- momentum_out: float32 [2048, 8192], P('shard', 'replica')
- params: bfloat16 [1024, 8192], P(None, 'replica')
The draws below stay inside these ranges and needn't reach their ends.
Inputs may be any that keep to these rules, and one draw needn't show every extreme that they name: `block_owner`: every shard owns at least one block and at most 4; some shard owns exactly 4. Rows of slots that are not live hold arbitrary deltas.
All inputs are finite; a program needn't handle non-finite values.
Results may differ from the reference program's by a relative error of at most 0.01.
Values may be sent and summed in bfloat16 or wider, within the bound.
A program may use at most 128 MiB of HBM per device.

```python
import math
import jax
import jax.numpy as jnp
import numpy as np
from jax import lax

D = 8192
BLOCK_ROWS = 128
SLOTS = 4
BLOCKS = 8
N_REPLICA = 8
N_SHARD = 4


def draw_deltas(key, part):
    rows = N_SHARD * SLOTS * BLOCK_ROWS
    base = jax.random.normal(key, (N_REPLICA, rows, D), jnp.float32)
    ramp = jnp.exp(jnp.log(3.0) * jnp.arange(rows, dtype=jnp.float32) / max(rows - 1, 1))
    rising = jnp.exp(jnp.log(3.0) * jnp.arange(N_REPLICA, dtype=jnp.float32) / max(N_REPLICA - 1, 1))
    column_ramp = jnp.exp(jnp.log(3.0) * jnp.arange(D, dtype=jnp.float32) / max(D - 1, 1))
    values = base * column_ramp[None, None, :]
    return (4.0 * values * ramp[None, :, None] * rising[:, None, None]).astype(jnp.bfloat16)


def levels(key, shape, cuts, smallest, largest):
    level, own = 1.0, jax.random.fold_in(key, 6)
    for dim, blocks in cuts:
        draws = jnp.exp(jax.random.uniform(jax.random.fold_in(own, dim), (blocks,), jnp.float32, smallest / len(cuts), largest / len(cuts)))
        level = level * jnp.repeat(draws, shape[dim] // blocks).reshape([-1 if axis == dim else 1 for axis in range(len(shape))])
    return level


def shared_out(own_key, own, number, rows, count, top, reach, slope):
    sequence = jax.random.permutation(own_key, count)
    packed, usual = load_shares(count, rows * top, reach, slope, True), load_shares(count, rows * top, reach, slope, False)
    places = jnp.arange(count)

    def named(lengths, offset_by):
        used = int((lengths > 0).sum())
        fixed = max(1, used // 4)
        moved = fixed + (places - fixed + offset_by * (used - fixed)) % max(1, count - fixed)
        return jnp.zeros((count,), jnp.int32).at[sequence[jnp.where(places < fixed, places, moved)]].set(jnp.asarray(lengths, jnp.int32))

    lengths = jnp.where(number % 4 == 0, named(packed, number // 4), named(usual, number - number // 4 - 1))
    mixed = jax.random.permutation(jax.random.fold_in(own, 3), count)
    giver, sink = mixed[0:count // 2 * 2:2], mixed[1:count // 2 * 2:2]
    slack = jnp.minimum(lengths[giver] - 1, reach - lengths[sink]) // 2
    slack = jnp.where((giver == sequence[0]) | (sink == sequence[0]) | (lengths[sink] == 0), 0, jnp.maximum(slack, 0))
    moved = jax.random.randint(jax.random.fold_in(own, 4), (count // 2,), 0, 1 << 20) % (slack + 1)
    lengths = lengths.at[giver].add(-moved).at[sink].add(moved)
    items = jnp.searchsorted(jnp.cumsum(lengths), jnp.arange(rows * top), side="right").astype(jnp.int32)
    table = items.reshape(top, rows).T
    table = table[jax.random.permutation(jax.random.fold_in(own, 1), rows)]
    offset_by = jax.random.randint(jax.random.fold_in(own, 2), (rows, 1), 0, top)
    return jnp.take_along_axis(table, (jnp.arange(top)[None, :] + offset_by) % top, axis=1)


def load_shares(number_of, total, reach, skew, full):
    loads = [(1 << 20) // math.isqrt(grade ** skew) + 1 for grade in range(1, number_of + 1)]
    largest = reach if full else min(reach, max(-(-total // number_of), total * loads[0] // sum(loads)))
    least = 1 if total - largest >= number_of - 1 else 0
    given, spare = [largest] + [least] * (number_of - 1), total - largest - least * (number_of - 1)
    while spare > 0:
        candidates = [i for i in range(1, number_of) if given[i] < largest] or [i for i in range(1, number_of) if given[i] < reach]
        whole, left = sum([loads[i] for i in candidates]), spare
        for i in candidates:
            more = min(reach - given[i], max(1, left * loads[i] // whole), spare)
            given[i] = given[i] + more
            spare = spare - more
    return np.array(given)


def normal_values(key, extent, deviation, most, cuts=(), held_as=jnp.bfloat16):
    gain = levels(key, extent, cuts, -0.22, 0.18) if cuts else 1.0
    result = jax.random.normal(key, extent, jnp.float32) * deviation * gain
    return jnp.minimum(jnp.maximum(result, -most), most).astype(held_as)


def setup_inputs(seed: int = 0) -> dict:
    arg_keys = jax.random.split(jax.random.key(seed), 5)
    deltas = draw_deltas(jax.random.fold_in(arg_keys[4], 71), 0)
    master = normal_values(arg_keys[1], (N_SHARD * SLOTS * BLOCK_ROWS, D), 1.0, 6.0, ((0, 4), (1, 8)), jnp.float32)
    momentum = normal_values(arg_keys[2], (N_SHARD * SLOTS * BLOCK_ROWS, D), 1.0, 6.0, ((0, 4), (1, 8)), jnp.float32)
    block_owner_keys = jax.random.split(jax.random.fold_in(arg_keys[3], 1), BLOCKS // BLOCKS)
    block_owner_turns = jax.random.permutation(jax.random.fold_in(arg_keys[3], 3), BLOCKS // BLOCKS)
    block_owner = jax.vmap(lambda own, number: shared_out(jax.random.fold_in(arg_keys[3], 2), own, number, BLOCKS, N_SHARD, 1, SLOTS, 2))(block_owner_keys, block_owner_turns).reshape((BLOCKS, 1))
    return dict(deltas=deltas, master=master, momentum=momentum, block_owner=block_owner)


def reference(deltas, master, momentum, block_owner):
    owner = block_owner[:, 0]
    shard_ids = jnp.arange(N_SHARD, dtype=jnp.int32)
    counts = lax.optimization_barrier(jnp.sum((owner[None, :] == shard_ids[:, None]).astype(jnp.int32), axis=1))
    live = jnp.arange(SLOTS, dtype=jnp.int32)[None, :] < counts[:, None]
    live_rows = jnp.repeat(live.reshape(-1), BLOCK_ROWS)[:, None]

    def add_one(total, piece):
        return (total + piece.astype(jnp.float32), None)
    summed, _ = lax.scan(add_one, jnp.zeros(master.shape, jnp.float32), deltas)
    avg = jnp.where(live_rows, summed / N_REPLICA, jnp.float32(0.0))
    total = jnp.sum(avg * avg)
    limit = 0.5 * jnp.sqrt(jnp.float32(BLOCKS * BLOCK_ROWS * D))
    factor = jnp.minimum(jnp.float32(1.0), limit / (jnp.sqrt(total) + 1e-06))
    grad = factor * avg
    momentum_out = jnp.where(live_rows, 0.9 * momentum + grad, momentum)
    master_out = jnp.where(live_rows, master - 0.7 * (grad + 0.9 * momentum_out), master)
    index = jnp.arange(BLOCKS, dtype=jnp.int32)
    same = (owner[None, :] == owner[:, None]) & (index[None, :] < index[:, None])
    before = lax.optimization_barrier(jnp.sum(same.astype(jnp.int32), axis=1))
    flat = (owner * SLOTS + before).astype(jnp.int32)
    blocks = master_out.reshape(N_SHARD * SLOTS, BLOCK_ROWS, D)[flat]
    params = blocks.astype(jnp.bfloat16).reshape(BLOCKS * BLOCK_ROWS, D)
    return (master_out, momentum_out, params)
```

```python
import functools

import jax
import jax.numpy as jnp
from jax import lax
from jax.experimental import pallas as pl
from jax.experimental.pallas import tpu as pltpu
from jax.sharding import PartitionSpec as P

BLOCK_ROWS = 128
SLOTS = 4
F32 = jnp.float32
BF16 = jnp.bfloat16
VMEM_LIMIT = 56 * 1024 * 1024


def remote(src, dst, send, recv, device):
    return pltpu.make_async_remote_copy(
        src_ref=src, dst_ref=dst, send_sem=send, recv_sem=recv,
        device_id=device, device_id_type=pl.DeviceIdType.MESH,
    )


def sync_kernel(
    R, S, held, rc,
    flags, deltas, base,
    sums, bases, tot,
    dv, p3, xin, pair, zin, mine, norm, nbuf, sbuf,
    ld, p3_s, p3_r, x_s, x_r, z_s, z_r, l_s, c_s, c_r, y_s, y_r, f_s, f_r,
    bl_s, bc_s, bc_r, by_s, by_r, bf_s, bf_r, n_s, n_r, m_s, m_r,
):
    width = deltas.shape[2]
    cols = width // R
    Z, O = R // 2, S // 2
    per = BLOCK_ROWS // rc
    chunks = held * per
    balanced = held < SLOTS
    direct = (held - 1 if balanced else held) * per
    me_r, me_s = lax.axis_index("replica"), lax.axis_index("shard")
    z, x = me_r // 2, me_r % 2
    o, core = me_s // 2, me_s % 2
    x_peer = z * 2 + 1 - x
    twin = o * 2 + 1 - core

    barrier = pltpu.get_barrier_semaphore()
    for i in range(1, R):
        pl.semaphore_signal(barrier, inc=1, device_id=((me_r + i) % R, me_s), device_id_type=pl.DeviceIdType.MESH)
    for i in range(1, S):
        pl.semaphore_signal(barrier, inc=1, device_id=(me_r, (me_s + i) % S), device_id_type=pl.DeviceIdType.MESH)

    def load(k):
        return pltpu.make_async_copy(
            deltas.at[0, pl.ds(k * BLOCK_ROWS, BLOCK_ROWS), :], dv.at[pl.ds(k * BLOCK_ROWS, BLOCK_ROWS), :], ld.at[k]
        )

    for k in reversed(range(held)):
        load(k).start()
    base_local = pltpu.make_async_copy(base, bases.at[me_s], bl_s)
    base_local.start()
    pl.semaphore_wait(barrier, R + S - 2)

    def rows_of(c):
        return pl.ds(pl.multiple_of(c * rc, rc), rc)

    def columns(c, j, side):
        return pl.ds(pl.multiple_of((((z + 1 + j) % Z) * 2 + side) * cols, cols), cols)

    def x_copy(source, c, j):
        return remote(
            source.at[rows_of(c), columns(c, j, 1 - x)], xin.at[c, j], x_s.at[c, j], x_r.at[c, j], (x_peer, me_s)
        )

    def z_copy(c, j):
        return remote(
            pair.at[c, j], zin.at[c, j], z_s.at[c, j], z_r.at[c, j], (((z + 1 + j) % Z) * 2 + x, me_s)
        )

    def c_copy(c):
        return remote(mine.at[c], sums.at[me_s, c], c_s.at[c], c_r.at[c], (me_r, twin))

    def l_copy(c):
        return pltpu.make_async_copy(mine.at[c], sums.at[me_s, c], l_s.at[c])

    def y_copy(i, c):
        return remote(
            mine.at[c], sums.at[me_s, c], y_s.at[i - 1, c], y_r.at[i - 1, c], (me_r, ((o + i) % O) * 2 + core)
        )

    def f_copy(i, c):
        source = ((o + O - i) % O) * 2 + core
        return remote(sums.at[source, c], sums.at[source, c], f_s.at[i - 1, c], f_r.at[i - 1, c], (me_r, twin))

    def by_copy(i):
        return remote(base, bases.at[me_s], by_s.at[i - 1], by_r.at[i - 1], (me_r, ((o + i) % O) * 2 + core))

    def bf_copy(i):
        source = ((o + O - i) % O) * 2 + core
        return remote(bases.at[source], bases.at[source], bf_s.at[i - 1], bf_r.at[i - 1], (me_r, twin))

    def third_copy():
        return remote(
            deltas.at[0, pl.ds((SLOTS - 1) * BLOCK_ROWS, BLOCK_ROWS), :], p3, p3_s, p3_r, (me_r, twin)
        )

    def base_twin():
        return remote(base, bases.at[me_s], bc_s, bc_r, (me_r, twin))

    def start_x(source, low, high):
        @pl.loop(low, high)
        def _(c):
            for j in range(Z):
                x_copy(source, c, j).start()

    start_x(deltas.at[0], 0, direct)
    if balanced:
        third_copy().start()
    for i in range(1, O):
        by_copy(i).start()
    base_twin().start()

    if balanced:
        load(held - 1).wait()
        third_copy().wait_recv()
        top = (held - 1) * BLOCK_ROWS

        @pl.loop(0, BLOCK_ROWS // 16)
        def _(r):
            own_flag = jnp.full((16, 1024), flags[0], jnp.int32) != 0
            for q in range(width // 1024):
                at = (pl.ds(pl.multiple_of(top + r * 16, 16), 16), pl.ds(q * 1024, 1024))
                other = (pl.ds(pl.multiple_of(r * 16, 16), 16), pl.ds(q * 1024, 1024))
                picked = jnp.where(own_flag, dv[at].astype(F32), p3[other].astype(F32))
                dv[at] = picked.astype(BF16)

        start_x(dv, direct, chunks)

    norm[0] = jnp.zeros((8, 128), F32)

    def add_pair(c):
        @pl.when(c % per == 0)
        def _():
            @pl.when(c < direct)
            def _():
                load(c // per).wait()

        for j in range(Z):
            x_copy(deltas.at[0], c, j).wait_recv()
            pair[c, j] = (xin[c, j].astype(F32) + dv[rows_of(c), columns(c, j, x)].astype(F32)).astype(BF16)
            if j < Z - 1:
                z_copy(c, j).start()

    def add_line(c):
        for j in range(Z - 1):
            z_copy(c, j).wait_recv()
        live = jnp.full((8, 128), flags[1 + c // per], jnp.int32) != 0
        part = jnp.zeros((8, 128), F32)
        for r in range(0, rc, 16):
            total = pair[c, Z - 1, r:r + 16, :].astype(F32)
            for j in range(Z - 1):
                total = total + zin[c, j, r:r + 16, :].astype(F32)
            total = total / R
            mine[c, r:r + 16, :] = total.astype(BF16)
            for h in range(0, 16, 8):
                for q in range(0, cols, 128):
                    v = total[h:h + 8, q:q + 128]
                    part = part + v * v
        norm[0] = norm[0] + jnp.where(live, part, 0.0)
        l_copy(c).start()
        for i in range(1, O):
            y_copy(i, c).start()
        c_copy(c).start()

    def forward(c):
        for i in range(1, O):
            y_copy(i, c).wait_recv()
            f_copy(i, c).start()

    lag2, lag3 = 2, 4

    @pl.loop(0, chunks + lag2)
    def _(t):
        @pl.when(t < chunks)
        def _():
            add_pair(t)

        @pl.when(t >= lag2)
        def _():
            add_line(t - lag2)

        @pl.when(t >= lag3)
        def _():
            forward(t - lag3)

        @pl.when(t == chunks // 2)
        def _():
            for i in range(1, O):
                by_copy(i).wait_recv()
                bf_copy(i).start()

    def n_copy(i):
        return remote(norm.at[0], nbuf.at[i - 1], n_s.at[i - 1], n_r.at[i - 1], ((me_r + i) % R, me_s))

    def m_copy(i):
        return remote(norm.at[1], sbuf.at[i - 1], m_s.at[i - 1], m_r.at[i - 1], (me_r, (me_s + i) % S))

    for i in range(1, R):
        n_copy(i).start()

    @pl.loop(chunks + lag2 - lag3, chunks)
    def _(c):
        forward(c)

    total = norm[0]
    for i in range(1, R):
        n_copy(i).wait_recv()
        total = total + nbuf[i - 1]
    norm[1] = total
    for i in range(1, S):
        m_copy(i).start()
    for i in range(1, S):
        m_copy(i).wait_recv()
        total = total + sbuf[i - 1]
    tot[...] = total

    if balanced:
        third_copy().wait_send()
    base_local.wait()
    base_twin().wait()
    for i in range(1, O):
        by_copy(i).wait_send()
        bf_copy(i).wait()
    for i in range(1, R):
        n_copy(i).wait_send()
    for i in range(1, S):
        m_copy(i).wait_send()

    @pl.loop(0, chunks)
    def _(c):
        for j in range(Z):
            x_copy(deltas.at[0], c, j).wait_send()
        for j in range(Z - 1):
            z_copy(c, j).wait_send()
        l_copy(c).wait()
        c_copy(c).wait()
        for i in range(1, O):
            y_copy(i, c).wait_send()
            f_copy(i, c).wait()


def update_kernel(where, live, scale, master, momentum, total, master_out, momentum_out):
    alive = live[pl.program_id(0)] != 0

    @pl.when(alive)
    def _():
        grad = scale[0] * total[0].astype(F32)
        fresh = 0.9 * momentum[...] + grad
        momentum_out[...] = fresh
        master_out[...] = master[...] - 0.7 * (grad + 0.9 * fresh)

    @pl.when(jnp.logical_not(alive))
    def _():
        momentum_out[...] = momentum[...]
        master_out[...] = master[...]


def place_kernel(from_base, from_sum, scale, base, total, out):
    grad = scale[0] * total[0].astype(F32)
    out[...] = (base[0].astype(F32) - 1.33 * grad).astype(BF16)


def on_device(deltas, master, momentum, block_owner):
    R, S = lax.axis_size("replica"), lax.axis_size("shard")
    me_shard = lax.axis_index("shard")
    width, cols = deltas.shape[2], master.shape[1]
    owner = block_owner[:, 0]
    blocks = owner.shape[0]
    most = min(2 * SLOTS, blocks - (S - 2))
    held = SLOTS - 1 if most <= 2 * (SLOTS - 1) else SLOTS
    balanced = held < SLOTS
    rc = BLOCK_ROWS
    while rc > 32 and held * (BLOCK_ROWS // (rc // 2)) * R <= 128:
        rc //= 2
    chunks = held * (BLOCK_ROWS // rc)
    Z, O = R // 2, S // 2

    count = jnp.sum((owner == me_shard).astype(jnp.int32))
    twin_count = jnp.sum((owner == (me_shard ^ 1)).astype(jnp.int32))
    slot = jnp.arange(SLOTS, dtype=jnp.int32)
    live = (slot < count).astype(jnp.int32)
    own_last = (count >= SLOTS - 1).astype(jnp.int32)
    work = live[:held]
    if balanced:
        last = jnp.where(own_last != 0, 1, (twin_count >= SLOTS).astype(jnp.int32))
        work = jnp.where(jnp.arange(held) == held - 1, last, work)
    flags = jnp.concatenate([own_last[None], work]).astype(jnp.int32)
    base = (master - 0.567 * momentum).astype(BF16)

    dma = pltpu.SemaphoreType.DMA
    ys = max(O - 1, 1)
    sums, bases, tot = pl.pallas_call(
        functools.partial(sync_kernel, R, S, held, rc),
        out_shape=(
            jax.ShapeDtypeStruct((S, chunks, rc, cols), BF16),
            jax.ShapeDtypeStruct((S,) + base.shape, BF16),
            jax.ShapeDtypeStruct((8, 128), F32),
        ),
        in_specs=[
            pl.BlockSpec(memory_space=pltpu.SMEM),
            pl.BlockSpec(memory_space=pl.ANY),
            pl.BlockSpec(memory_space=pltpu.VMEM),
        ],
        out_specs=(
            pl.BlockSpec(memory_space=pl.ANY),
            pl.BlockSpec(memory_space=pl.ANY),
            pl.BlockSpec(memory_space=pltpu.VMEM),
        ),
        scratch_shapes=[
            pltpu.VMEM((held * BLOCK_ROWS, width), BF16),
            pltpu.VMEM((BLOCK_ROWS, width) if balanced else (16, 128), BF16),
            pltpu.VMEM((chunks, Z, rc, cols), BF16),
            pltpu.VMEM((chunks, Z, rc, cols), BF16),
            pltpu.VMEM((chunks, max(Z - 1, 1), rc, cols), BF16),
            pltpu.VMEM((chunks, rc, cols), BF16),
            pltpu.VMEM((2, 8, 128), F32),
            pltpu.VMEM((R - 1, 8, 128), F32),
            pltpu.VMEM((S - 1, 8, 128), F32),
            dma((held,)), dma, dma,
            dma((chunks, Z)), dma((chunks, Z)),
            dma((chunks, max(Z - 1, 1))), dma((chunks, max(Z - 1, 1))),
            dma((chunks,)), dma((chunks,)), dma((chunks,)),
            dma((ys, chunks)), dma((ys, chunks)), dma((ys, chunks)), dma((ys, chunks)),
            dma, dma, dma,
            dma((ys,)), dma((ys,)), dma((ys,)), dma((ys,)),
            dma((R - 1,)), dma((R - 1,)), dma((S - 1,)), dma((S - 1,)),
        ],
        compiler_params=pltpu.CompilerParams(
            collective_id=0, has_side_effects=True, vmem_limit_bytes=VMEM_LIMIT
        ),
        name="sync",
    )(flags, deltas, base)

    total = jnp.sum(tot)
    limit = 0.5 * jnp.sqrt(F32(blocks * BLOCK_ROWS * width))
    factor = jnp.minimum(F32(1.0), limit / (jnp.sqrt(total) + 1e-06))
    scale = factor[None]
    sums = sums.reshape(S * held, BLOCK_ROWS, cols)
    bases = bases.reshape(S * SLOTS, BLOCK_ROWS, cols)

    def sum_at(shard, place):
        if not balanced:
            return shard * held + place
        return jnp.where(place < held, shard * held + place, (shard ^ 1) * held + held - 1)

    def block(index_map, lead=True):
        return pl.BlockSpec(((1,) if lead else ()) + (BLOCK_ROWS, cols), index_map)

    master_out, momentum_out = pl.pallas_call(
        update_kernel,
        out_shape=(jax.ShapeDtypeStruct(master.shape, F32),) * 2,
        grid_spec=pltpu.PrefetchScalarGridSpec(
            num_scalar_prefetch=3,
            grid=(SLOTS,),
            in_specs=[
                block(lambda i, w, l, f: (i, 0), False),
                block(lambda i, w, l, f: (i, 0), False),
                block(lambda i, w, l, f: (w[i], 0, 0)),
            ],
            out_specs=(block(lambda i, w, l, f: (i, 0), False),) * 2,
        ),
        name="update",
    )(sum_at(me_shard, slot).astype(jnp.int32), live, scale, master, momentum, sums)

    index = jnp.arange(blocks, dtype=jnp.int32)
    same = (owner[None, :] == owner[:, None]) & (index[None, :] < index[:, None])
    before = jnp.sum(same.astype(jnp.int32), axis=1)
    params = pl.pallas_call(
        place_kernel,
        out_shape=jax.ShapeDtypeStruct((blocks * BLOCK_ROWS, cols), BF16),
        grid_spec=pltpu.PrefetchScalarGridSpec(
            num_scalar_prefetch=3,
            grid=(blocks,),
            in_specs=[
                block(lambda i, b, s, f: (b[i], 0, 0)),
                block(lambda i, b, s, f: (s[i], 0, 0)),
            ],
            out_specs=block(lambda i, b, s, f: (i, 0), False),
        ),
        name="place",
    )((owner * SLOTS + before).astype(jnp.int32), sum_at(owner, before).astype(jnp.int32), scale, bases, sums)
    return (master_out, momentum_out, params)


def solution(mesh):
    return jax.shard_map(
        on_device,
        mesh=mesh,
        in_specs=(P("replica", "shard", None), P("shard", "replica"), P("shard", "replica"), P()),
        out_specs=(P("shard", "replica"), P("shard", "replica"), P(None, "replica")),
        check_vma=False,
    )
```

```python
import functools

import jax
import jax.numpy as jnp
from jax import lax
from jax.experimental import pallas as pl
from jax.experimental.pallas import tpu as pltpu
from jax.sharding import PartitionSpec as P

BLOCK_ROWS = 128
SLOTS = 4
F32 = jnp.float32
BF16 = jnp.bfloat16
VMEM_LIMIT = 56 * 1024 * 1024


def remote(src, dst, send, recv, device):
    return pltpu.make_async_remote_copy(
        src_ref=src, dst_ref=dst, send_sem=send, recv_sem=recv,
        device_id=device, device_id_type=pl.DeviceIdType.MESH,
    )


def shard_count(owner, shard):
    return sum(jnp.where(owner[b, 0] == shard, 1, 0) for b in range(owner.shape[0]))


def spread(condition, shape):
    return jnp.full(shape, jnp.where(condition, 1, 0), jnp.int32) != 0


def sync_kernel(
    R, S, rows, rc,
    owner, deltas, master, momentum,
    sums, bases, tot,
    dv, p3, yt, ms, mm, base, xin, pair, zin, mine, norm, nbuf, sbuf,
    ld, lm, p3_s, p3_r, t_s, t_r, x_s, x_r, z_s, z_r, l_s, c_s, c_r, y_s, y_r, f_s, f_r,
    bl_s, bc_s, bc_r, by_s, by_r, bf_s, bf_r, n_s, n_r, m_s, m_r,
):
    width = deltas.shape[2]
    cols = width // R
    Z, O = R // 2, S // 2
    per = BLOCK_ROWS // rc
    half = BLOCK_ROWS // 2
    chunks = rows // rc
    quad = rows < SLOTS * BLOCK_ROWS
    whole = rows // BLOCK_ROWS
    direct = whole * per
    top = whole * BLOCK_ROWS
    me_r, me_s = lax.axis_index("replica"), lax.axis_index("shard")
    z, x = me_r // 2, me_r % 2
    o, core = me_s // 2, me_s % 2
    x_peer = z * 2 + 1 - x
    twin = o * 2 + 1 - core

    barrier = pltpu.get_barrier_semaphore()
    for i in range(1, R):
        pl.semaphore_signal(barrier, inc=1, device_id=((me_r + i) % R, me_s), device_id_type=pl.DeviceIdType.MESH)
    for i in range(1, S):
        pl.semaphore_signal(barrier, inc=1, device_id=(me_r, (me_s + i) % S), device_id_type=pl.DeviceIdType.MESH)

    def load(k):
        part = pl.ds(k * BLOCK_ROWS, BLOCK_ROWS)
        return pltpu.make_async_copy(deltas.at[0, part, :], dv.at[part, :], ld.at[k])

    if quad:
        load(whole).start()
    for k in range(whole):
        load(k).start()
    load_master = pltpu.make_async_copy(master, ms, lm.at[0])
    load_momentum = pltpu.make_async_copy(momentum, mm, lm.at[1])
    load_master.start()
    load_momentum.start()
    mine_count = shard_count(owner, me_s)
    twin_count = shard_count(owner, twin)
    heavy = jnp.maximum(mine_count, twin_count) >= SLOTS
    pl.semaphore_wait(barrier, R + S - 2)

    def rows_of(c):
        return pl.ds(pl.multiple_of(c * rc, rc), rc)

    def columns(c, j, side):
        return pl.ds(pl.multiple_of((((z + 1 + j) % Z) * 2 + side) * cols, cols), cols)

    def x_copy(source, c, j):
        return remote(
            source.at[rows_of(c), columns(c, j, 1 - x)], xin.at[c, j], x_s.at[c, j], x_r.at[c, j], (x_peer, me_s)
        )

    def z_copy(c, j):
        return remote(
            pair.at[c, j], zin.at[c, j], z_s.at[c, j], z_r.at[c, j], (((z + 1 + j) % Z) * 2 + x, me_s)
        )

    def c_copy(c):
        return remote(mine.at[c], sums.at[me_s, c], c_s.at[c], c_r.at[c], (me_r, twin))

    def l_copy(c):
        return pltpu.make_async_copy(mine.at[c], sums.at[me_s, c], l_s.at[c])

    def y_copy(i, c):
        return remote(
            mine.at[c], sums.at[me_s, c], y_s.at[i - 1, c], y_r.at[i - 1, c], (me_r, ((o + i) % O) * 2 + core)
        )

    def f_copy(i, c):
        source = ((o + O - i) % O) * 2 + core
        return remote(sums.at[source, c], sums.at[source, c], f_s.at[i - 1, c], f_r.at[i - 1, c], (me_r, twin))

    def by_copy(i):
        return remote(base, bases.at[me_s], by_s.at[i - 1], by_r.at[i - 1], (me_r, ((o + i) % O) * 2 + core))

    def bf_copy(i):
        source = ((o + O - i) % O) * 2 + core
        return remote(bases.at[source], bases.at[source], bf_s.at[i - 1], bf_r.at[i - 1], (me_r, twin))

    def third_copy(h):
        return remote(
            deltas.at[0, pl.ds((SLOTS - 1) * BLOCK_ROWS + h * half, half), :],
            p3.at[pl.ds(h * half, half), :], p3_s.at[h], p3_r.at[h], (me_r, twin),
        )

    def t_copy():
        return remote(dv.at[pl.ds(top + half, half), :], yt, t_s, t_r, (me_r, ((o + 1) % O) * 2 + core))

    def base_twin():
        return remote(base, bases.at[me_s], bc_s, bc_r, (me_r, twin))

    def base_local():
        return pltpu.make_async_copy(base, bases.at[me_s], bl_s)

    def start_x(source, low, high):
        @pl.loop(low, high)
        def _(c):
            for j in range(Z):
                x_copy(source, c, j).start()

    def pick(condition, other, start, other_start):
        @pl.loop(0, half // 16)
        def _(r):
            keep = spread(condition, (16, 1024))
            for q in range(width // 1024):
                at = (pl.ds(pl.multiple_of(start + r * 16, 16), 16), pl.ds(q * 1024, 1024))
                there = (pl.ds(pl.multiple_of(other_start + r * 16, 16), 16), pl.ds(q * 1024, 1024))
                dv[at] = jnp.where(keep, dv[at].astype(F32), other[there].astype(F32)).astype(BF16)

    if quad:
        third_copy(1).start()
        third_copy(0).start()
    start_x(deltas.at[0], 0, direct)
    norm[0] = jnp.zeros((8, 128), F32)
    if quad:
        load(whole).wait()
        third_copy(1).wait_recv()
        pick(mine_count >= SLOTS, p3, top + half, half)
        t_copy().start()

    def make_base():
        load_master.wait()
        load_momentum.wait()

        @pl.loop(0, SLOTS * BLOCK_ROWS // 16)
        def _(r):
            at = pl.ds(pl.multiple_of(r * 16, 16), 16)
            base[at, :] = (ms[at, :] - 0.567 * mm[at, :]).astype(BF16)

        for i in range(1, O):
            by_copy(i).start()
        base_twin().start()
        base_local().start()

    def add_pair(c):
        @pl.when(c % per == 0)
        def _():
            @pl.when(c < direct)
            def _():
                load(c // per).wait()

        for j in range(Z):
            x_copy(deltas.at[0], c, j).wait_recv()
            pair[c, j] = (xin[c, j].astype(F32) + dv[rows_of(c), columns(c, j, x)].astype(F32)).astype(BF16)
            if j < Z - 1:
                z_copy(c, j).start()

    def add_line(c):
        for j in range(Z - 1):
            z_copy(c, j).wait_recv()
        live = c // per < mine_count
        if quad:
            live = jnp.logical_or(live, c >= direct)
        live = spread(live, (8, 128))
        part = jnp.zeros((8, 128), F32)
        for r in range(0, rc, 16):
            total = pair[c, Z - 1, r:r + 16, :].astype(F32)
            for j in range(Z - 1):
                total = total + zin[c, j, r:r + 16, :].astype(F32)
            total = total / R
            mine[c, r:r + 16, :] = total.astype(BF16)
            for h in range(0, 16, 8):
                for q in range(0, cols, 128):
                    v = total[h:h + 8, q:q + 128]
                    part = part + v * v
        norm[0] = norm[0] + jnp.where(live, part, 0.0)
        for i in range(1, O):
            y_copy(i, c).start()
        c_copy(c).start()
        l_copy(c).start()

    def forward(c):
        for i in range(1, O):
            y_copy(i, c).wait_recv()
            f_copy(i, c).start()

    lag = 4

    @pl.loop(0, chunks + lag)
    def _(t):
        @pl.when(t < chunks)
        def _():
            add_pair(t)

        @pl.when(t >= lag)
        def _():
            add_line(t - lag)

        @pl.when(t == 1)
        def _():
            make_base()

        if quad:
            @pl.when(t == direct - direct // 4)
            def _():
                third_copy(0).wait_recv()
                pick(mine_count >= SLOTS, p3, top, 0)
                t_copy().wait_recv()
                pick(heavy, yt, top, 0)
                start_x(dv, direct, chunks)

    def n_copy(i):
        return remote(norm.at[0], nbuf.at[i - 1], n_s.at[i - 1], n_r.at[i - 1], ((me_r + i) % R, me_s))

    def m_copy(i):
        return remote(norm.at[1], sbuf.at[i - 1], m_s.at[i - 1], m_r.at[i - 1], (me_r, (me_s + i) % S))

    for i in range(1, R):
        n_copy(i).start()
    for i in range(1, O):
        by_copy(i).wait_recv()
        bf_copy(i).start()

    @pl.loop(0, chunks - 2)
    def _(c):
        forward(c)

    total = norm[0]
    for i in range(1, R):
        n_copy(i).wait_recv()
        total = total + nbuf[i - 1]
    norm[1] = total
    for i in range(1, S):
        m_copy(i).start()

    @pl.loop(chunks - 2, chunks)
    def _(c):
        forward(c)

    for i in range(1, S):
        m_copy(i).wait_recv()
        total = total + sbuf[i - 1]
    tot[...] = total

    if quad:
        third_copy(0).wait_send()
        third_copy(1).wait_send()
        t_copy().wait_send()
    base_local().wait()
    base_twin().wait()
    for i in range(1, O):
        by_copy(i).wait_send()
        bf_copy(i).wait()
    for i in range(1, R):
        n_copy(i).wait_send()
    for i in range(1, S):
        m_copy(i).wait_send()

    @pl.loop(0, chunks)
    def _(c):
        for j in range(Z):
            x_copy(deltas.at[0], c, j).wait_send()
        for j in range(Z - 1):
            z_copy(c, j).wait_send()
        l_copy(c).wait()
        c_copy(c).wait()
        for i in range(1, O):
            y_copy(i, c).wait_send()
            f_copy(i, c).wait()


def finish_kernel(
    R, units,
    owner, tot, master, momentum, sums, bases,
    master_out, momentum_out, params,
    ms, mm, su, pb, ps,
    a_s, b_s, u_s, p_s, q_s, oa_s, ob_s, op_s,
):
    blocks = owner.shape[0]
    cols = master.shape[1]
    half = BLOCK_ROWS // 2
    me_s = lax.axis_index("shard")
    count = shard_count(owner, me_s)

    def unit(shard, place, h):
        if units == 2 * SLOTS:
            return shard * units + 2 * place + h
        moved = shard + jnp.where(place == SLOTS - 1, 1 - 2 * (shard % 2), 0)
        if h:
            moved = moved + jnp.where(moved // 2 == 0, 2, -2)
        return jnp.where(place < 2, shard * units + 2 * place + h, moved * units + units - 1)

    def slot_rows(j):
        return pl.ds(pl.multiple_of(j * BLOCK_ROWS, BLOCK_ROWS), BLOCK_ROWS)

    def get_slot(j):
        return [
            pltpu.make_async_copy(master.at[slot_rows(j)], ms.at[slot_rows(j)], a_s.at[j]),
            pltpu.make_async_copy(momentum.at[slot_rows(j)], mm.at[slot_rows(j)], b_s.at[j]),
        ] + [
            pltpu.make_async_copy(sums.at[unit(me_s, j, h)], su.at[2 * j + h], u_s.at[2 * j + h]) for h in range(2)
        ]

    def put_slot(j):
        return [
            pltpu.make_async_copy(ms.at[slot_rows(j)], master_out.at[slot_rows(j)], oa_s.at[j]),
            pltpu.make_async_copy(mm.at[slot_rows(j)], momentum_out.at[slot_rows(j)], ob_s.at[j]),
        ]

    def get_block(b):
        shard = owner[b, 0]
        place = sum(jnp.where(jnp.logical_and(owner[k, 0] == shard, k < b), 1, 0) for k in range(blocks))
        return [pltpu.make_async_copy(bases.at[shard * SLOTS + place], pb.at[b], p_s.at[b])] + [
            pltpu.make_async_copy(sums.at[unit(shard, place, h)], ps.at[2 * b + h], q_s.at[2 * b + h])
            for h in range(2)
        ]

    def put_block(b):
        return pltpu.make_async_copy(pb.at[b], params.at[slot_rows(b)], op_s.at[b])

    @pl.loop(0, SLOTS)
    def _(j):
        for copy in get_slot(j):
            copy.start()

    @pl.loop(0, blocks)
    def _(b):
        for copy in get_block(b):
            copy.start()

    total = jnp.sum(jnp.sum(tot[...], axis=1, keepdims=True), axis=0, keepdims=True)
    limit = 0.5 * jnp.sqrt(jnp.full((1, 1), blocks * BLOCK_ROWS * R * cols, F32))
    factor = jnp.minimum(1.0, limit / (jnp.sqrt(total) + 1e-06))

    @pl.loop(0, SLOTS)
    def _(j):
        for copy in get_slot(j):
            copy.wait()

        @pl.when(j < count)
        def _():
            for h in range(2):
                @pl.loop(0, half // 16)
                def _(r):
                    at = pl.ds(pl.multiple_of(j * BLOCK_ROWS + h * half + r * 16, 16), 16)
                    grad = factor * su[2 * j + h, pl.ds(pl.multiple_of(r * 16, 16), 16), :].astype(F32)
                    fresh = 0.9 * mm[at, :] + grad
                    mm[at, :] = fresh
                    ms[at, :] = ms[at, :] - 0.7 * (grad + 0.9 * fresh)

        for copy in put_slot(j):
            copy.start()

    @pl.loop(0, blocks)
    def _(b):
        for copy in get_block(b):
            copy.wait()
        for h in range(2):
            @pl.loop(0, half // 16)
            def _(r):
                at = pl.ds(pl.multiple_of(h * half + r * 16, 16), 16)
                grad = factor * ps[2 * b + h, pl.ds(pl.multiple_of(r * 16, 16), 16), :].astype(F32)
                pb[b, at, :] = (pb[b, at, :].astype(F32) - 1.33 * grad).astype(BF16)

        put_block(b).start()

    @pl.loop(0, SLOTS)
    def _(j):
        for copy in put_slot(j):
            copy.wait()

    @pl.loop(0, blocks)
    def _(b):
        put_block(b).wait()


def on_device(deltas, master, momentum, block_owner):
    R, S = lax.axis_size("replica"), lax.axis_size("shard")
    width, cols = deltas.shape[2], master.shape[1]
    blocks = block_owner.shape[0]
    half = BLOCK_ROWS // 2
    quad = S == 4 and blocks - SLOTS - (S - 2) <= 2
    rows = 2 * BLOCK_ROWS + half if quad else SLOTS * BLOCK_ROWS
    rc = half
    while rc > 16 and (rows // (rc // 2)) * R <= 160:
        rc //= 2
    chunks = rows // rc
    units = rows // half
    Z, O = R // 2, S // 2
    loads = rows // BLOCK_ROWS + (1 if quad else 0)

    dma = pltpu.SemaphoreType.DMA
    vmem = pltpu.VMEM
    anywhere = pl.BlockSpec(memory_space=pl.ANY)
    in_vmem = pl.BlockSpec(memory_space=pltpu.VMEM)
    in_smem = pl.BlockSpec(memory_space=pltpu.SMEM)
    ys, zs = max(O - 1, 1), max(Z - 1, 1)
    sums, bases, tot = pl.pallas_call(
        functools.partial(sync_kernel, R, S, rows, rc),
        out_shape=(
            jax.ShapeDtypeStruct((S, chunks, rc, cols), BF16),
            jax.ShapeDtypeStruct((S,) + master.shape, BF16),
            jax.ShapeDtypeStruct((8, 128), F32),
        ),
        in_specs=[in_smem, anywhere, anywhere, anywhere],
        out_specs=(anywhere, anywhere, in_vmem),
        scratch_shapes=[
            vmem((loads * BLOCK_ROWS, width), BF16),
            vmem((BLOCK_ROWS, width) if quad else (16, 128), BF16),
            vmem((half, width) if quad else (16, 128), BF16),
            vmem(master.shape, F32),
            vmem(master.shape, F32),
            vmem(master.shape, BF16),
            vmem((chunks, Z, rc, cols), BF16),
            vmem((chunks, Z, rc, cols), BF16),
            vmem((chunks, zs, rc, cols), BF16),
            vmem((chunks, rc, cols), BF16),
            vmem((2, 8, 128), F32),
            vmem((R - 1, 8, 128), F32),
            vmem((S - 1, 8, 128), F32),
            dma((loads,)), dma((2,)), dma((2,)), dma((2,)), dma, dma,
            dma((chunks, Z)), dma((chunks, Z)),
            dma((chunks, zs)), dma((chunks, zs)),
            dma((chunks,)), dma((chunks,)), dma((chunks,)),
            dma((ys, chunks)), dma((ys, chunks)), dma((ys, chunks)), dma((ys, chunks)),
            dma, dma, dma,
            dma((ys,)), dma((ys,)), dma((ys,)), dma((ys,)),
            dma((R - 1,)), dma((R - 1,)), dma((S - 1,)), dma((S - 1,)),
        ],
        compiler_params=pltpu.CompilerParams(
            collective_id=0, has_side_effects=True, vmem_limit_bytes=VMEM_LIMIT
        ),
        name="sync",
    )(block_owner, deltas, master, momentum)

    return tuple(pl.pallas_call(
        functools.partial(finish_kernel, R, units),
        out_shape=(
            jax.ShapeDtypeStruct(master.shape, F32),
            jax.ShapeDtypeStruct(master.shape, F32),
            jax.ShapeDtypeStruct((blocks * BLOCK_ROWS, cols), BF16),
        ),
        in_specs=[in_smem, in_vmem] + [anywhere] * 4,
        out_specs=(anywhere,) * 3,
        scratch_shapes=[
            vmem(master.shape, F32),
            vmem(master.shape, F32),
            vmem((2 * SLOTS, half, cols), BF16),
            vmem((blocks, BLOCK_ROWS, cols), BF16),
            vmem((2 * blocks, half, cols), BF16),
            dma((SLOTS,)), dma((SLOTS,)), dma((2 * SLOTS,)), dma((blocks,)), dma((2 * blocks,)),
            dma((SLOTS,)), dma((SLOTS,)), dma((blocks,)),
        ],
        compiler_params=pltpu.CompilerParams(vmem_limit_bytes=VMEM_LIMIT),
        name="finish",
    )(block_owner, tot, master, momentum, sums.reshape(S * units, half, cols),
      bases.reshape(S * SLOTS, BLOCK_ROWS, cols)))


def solution(mesh):
    return jax.shard_map(
        on_device,
        mesh=mesh,
        in_specs=(P("replica", "shard", None), P("shard", "replica"), P("shard", "replica"), P()),
        out_specs=(P("shard", "replica"), P("shard", "replica"), P(None, "replica")),
        check_vma=False,
    )
```

```python
import functools

import jax
import jax.numpy as jnp
from jax import lax
from jax.experimental import pallas as pl
from jax.experimental.pallas import tpu as pltpu
from jax.sharding import PartitionSpec as P

BLOCK_ROWS = 128
SLOTS = 4
F32 = jnp.float32
BF16 = jnp.bfloat16
VMEM_LIMIT = 56 * 1024 * 1024


def remote(src, dst, send, recv, device):
    return pltpu.make_async_remote_copy(
        src_ref=src, dst_ref=dst, send_sem=send, recv_sem=recv,
        device_id=device, device_id_type=pl.DeviceIdType.MESH,
    )


def shard_count(owner, shard):
    return sum(jnp.where(owner[b, 0] == shard, 1, 0) for b in range(owner.shape[0]))


def spread(condition, shape):
    return jnp.broadcast_to(jnp.where(condition, 1, 0), shape) != 0


def sync_kernel(
    R, S, rows, rc,
    owner, deltas, master, momentum,
    sums, bases, tot,
    dv, p3, yt, ms, mm, base, xin, pair, zin, mine, norm, nbuf, sbuf,
    ld, lm, p3_s, p3_r, t_s, t_r, x_s, x_r, z_s, z_r, l_s, c_s, c_r, y_s, y_r, f_s, f_r,
    bl_s, bc_s, bc_r, by_s, by_r, bf_s, bf_r, n_s, n_r, m_s, m_r,
):
    width = deltas.shape[2]
    cols = width // R
    Z, O = R // 2, S // 2
    per = BLOCK_ROWS // rc
    half = BLOCK_ROWS // 2
    chunks = rows // rc
    quad = rows < SLOTS * BLOCK_ROWS
    whole = rows // BLOCK_ROWS
    direct = whole * per
    top = whole * BLOCK_ROWS
    me_r, me_s = lax.axis_index("replica"), lax.axis_index("shard")
    z, x = me_r // 2, me_r % 2
    o, core = me_s // 2, me_s % 2
    x_peer = z * 2 + 1 - x
    twin = o * 2 + 1 - core

    barrier = pltpu.get_barrier_semaphore()
    for i in range(1, R):
        pl.semaphore_signal(barrier, inc=1, device_id=((me_r + i) % R, me_s), device_id_type=pl.DeviceIdType.MESH)
    for i in range(1, S):
        pl.semaphore_signal(barrier, inc=1, device_id=(me_r, (me_s + i) % S), device_id_type=pl.DeviceIdType.MESH)

    def load(k):
        part = pl.ds(k * BLOCK_ROWS, BLOCK_ROWS)
        return pltpu.make_async_copy(deltas.at[0, part, :], dv.at[part, :], ld.at[k])

    if quad:
        load(whole).start()
    for k in range(whole):
        load(k).start()
    load_master = pltpu.make_async_copy(master, ms, lm.at[0])
    load_momentum = pltpu.make_async_copy(momentum, mm, lm.at[1])
    load_master.start()
    load_momentum.start()
    mine_count = jnp.sum(jnp.where(owner[...] == me_s, 1, 0), axis=0, keepdims=True)
    twin_count = jnp.sum(jnp.where(owner[...] == twin, 1, 0), axis=0, keepdims=True)
    heavy = jnp.maximum(mine_count, twin_count) >= SLOTS
    pl.semaphore_wait(barrier, R + S - 2)

    def rows_of(c):
        return pl.ds(pl.multiple_of(c * rc, rc), rc)

    def columns(c, j, side):
        return pl.ds(pl.multiple_of((((z + 1 + j) % Z) * 2 + side) * cols, cols), cols)

    def x_copy(source, c, j):
        return remote(
            source.at[rows_of(c), columns(c, j, 1 - x)], xin.at[c, j], x_s.at[c, j], x_r.at[c, j], (x_peer, me_s)
        )

    def z_copy(c, j):
        return remote(
            pair.at[c, j], zin.at[c, j], z_s.at[c, j], z_r.at[c, j], (((z + 1 + j) % Z) * 2 + x, me_s)
        )

    def c_copy(c):
        return remote(mine.at[c], sums.at[me_s, c], c_s.at[c], c_r.at[c], (me_r, twin))

    def l_copy(c):
        return pltpu.make_async_copy(mine.at[c], sums.at[me_s, c], l_s.at[c])

    def y_copy(i, c):
        return remote(
            mine.at[c], sums.at[me_s, c], y_s.at[i - 1, c], y_r.at[i - 1, c], (me_r, ((o + i) % O) * 2 + core)
        )

    def f_copy(i, c):
        source = ((o + O - i) % O) * 2 + core
        return remote(sums.at[source, c], sums.at[source, c], f_s.at[i - 1, c], f_r.at[i - 1, c], (me_r, twin))

    def by_copy(i):
        return remote(base, bases.at[me_s], by_s.at[i - 1], by_r.at[i - 1], (me_r, ((o + i) % O) * 2 + core))

    def bf_copy(i):
        source = ((o + O - i) % O) * 2 + core
        return remote(bases.at[source], bases.at[source], bf_s.at[i - 1], bf_r.at[i - 1], (me_r, twin))

    def third_copy(h):
        return remote(
            deltas.at[0, pl.ds((SLOTS - 1) * BLOCK_ROWS + h * half, half), :],
            p3.at[pl.ds(h * half, half), :], p3_s.at[h], p3_r.at[h], (me_r, twin),
        )

    def t_copy():
        return remote(dv.at[pl.ds(top + half, half), :], yt, t_s, t_r, (me_r, ((o + 1) % O) * 2 + core))

    def base_twin():
        return remote(base, bases.at[me_s], bc_s, bc_r, (me_r, twin))

    def base_local():
        return pltpu.make_async_copy(base, bases.at[me_s], bl_s)

    def start_x(source, low, high):
        @pl.loop(low, high)
        def _(c):
            for j in range(Z):
                x_copy(source, c, j).start()

    def pick(condition, other, start, other_start):
        @pl.loop(0, half // 16)
        def _(r):
            keep = spread(condition, (16, 1024))
            for q in range(width // 1024):
                at = (pl.ds(pl.multiple_of(start + r * 16, 16), 16), pl.ds(q * 1024, 1024))
                there = (pl.ds(pl.multiple_of(other_start + r * 16, 16), 16), pl.ds(q * 1024, 1024))
                dv[at] = jnp.where(keep, dv[at].astype(F32), other[there].astype(F32)).astype(BF16)

    if quad:
        third_copy(1).start()
        third_copy(0).start()
    start_x(deltas.at[0], 0, direct)
    norm[0] = jnp.zeros((8, 128), F32)

    def send_third():
        load(whole).wait()
        third_copy(1).wait_recv()
        pick(mine_count >= SLOTS, p3, top + half, half)
        t_copy().start()

    def make_base():
        load_master.wait()
        load_momentum.wait()

        @pl.loop(0, SLOTS * BLOCK_ROWS // 16)
        def _(r):
            at = pl.ds(pl.multiple_of(r * 16, 16), 16)
            base[at, :] = (ms[at, :] - 0.567 * mm[at, :]).astype(BF16)

        for i in range(1, O):
            by_copy(i).start()
        base_twin().start()
        base_local().start()

    def add_pair(c):
        @pl.when(c % per == 0)
        def _():
            @pl.when(c < direct)
            def _():
                load(c // per).wait()

        for j in range(Z):
            x_copy(deltas.at[0], c, j).wait_recv()
            pair[c, j] = (xin[c, j].astype(F32) + dv[rows_of(c), columns(c, j, x)].astype(F32)).astype(BF16)
            if j < Z - 1:
                z_copy(c, j).start()

    def add_line(c):
        for j in range(Z - 1):
            z_copy(c, j).wait_recv()
        place = jnp.where(c >= direct, -1, c // per) if quad else c // per
        live = spread(place < mine_count, (8, 128))
        part = jnp.zeros((8, 128), F32)
        for r in range(0, rc, 16):
            total = pair[c, Z - 1, r:r + 16, :].astype(F32)
            for j in range(Z - 1):
                total = total + zin[c, j, r:r + 16, :].astype(F32)
            total = total / R
            mine[c, r:r + 16, :] = total.astype(BF16)
            for h in range(0, 16, 8):
                for q in range(0, cols, 128):
                    v = total[h:h + 8, q:q + 128]
                    part = part + v * v
        norm[0] = norm[0] + jnp.where(live, part, 0.0)
        for i in range(1, O):
            y_copy(i, c).start()
        c_copy(c).start()
        l_copy(c).start()

    def forward(c):
        for i in range(1, O):
            y_copy(i, c).wait_recv()
            f_copy(i, c).start()

    lag = 4

    @pl.loop(0, chunks + lag)
    def _(t):
        @pl.when(t < chunks)
        def _():
            add_pair(t)

        @pl.when(t >= lag)
        def _():
            add_line(t - lag)

        @pl.when(t == 2)
        def _():
            make_base()

        if quad:
            @pl.when(t == 0)
            def _():
                send_third()

            @pl.when(t == direct - direct // 4)
            def _():
                third_copy(0).wait_recv()
                pick(mine_count >= SLOTS, p3, top, 0)
                t_copy().wait_recv()
                pick(heavy, yt, top, 0)
                start_x(dv, direct, chunks)

    def n_copy(i):
        return remote(norm.at[0], nbuf.at[i - 1], n_s.at[i - 1], n_r.at[i - 1], ((me_r + i) % R, me_s))

    def m_copy(i):
        return remote(norm.at[1], sbuf.at[i - 1], m_s.at[i - 1], m_r.at[i - 1], (me_r, (me_s + i) % S))

    for i in range(1, R):
        n_copy(i).start()
    for i in range(1, O):
        by_copy(i).wait_recv()
        bf_copy(i).start()

    @pl.loop(0, chunks - 2)
    def _(c):
        forward(c)
        for j in range(Z):
            x_copy(deltas.at[0], c, j).wait_send()
        for j in range(Z - 1):
            z_copy(c, j).wait_send()

    total = norm[0]
    for i in range(1, R):
        n_copy(i).wait_recv()
        total = total + nbuf[i - 1]
    norm[1] = total
    for i in range(1, S):
        m_copy(i).start()

    @pl.loop(chunks - 2, chunks)
    def _(c):
        forward(c)

    for i in range(1, S):
        m_copy(i).wait_recv()
        total = total + sbuf[i - 1]
    tot[...] = total

    if quad:
        third_copy(0).wait_send()
        third_copy(1).wait_send()
        t_copy().wait_send()
    base_local().wait()
    base_twin().wait()
    for i in range(1, O):
        by_copy(i).wait_send()
        bf_copy(i).wait()
    for i in range(1, R):
        n_copy(i).wait_send()
    for i in range(1, S):
        m_copy(i).wait_send()

    @pl.loop(chunks - 2, chunks)
    def _(c):
        for j in range(Z):
            x_copy(deltas.at[0], c, j).wait_send()
        for j in range(Z - 1):
            z_copy(c, j).wait_send()

    @pl.loop(0, chunks)
    def _(c):
        l_copy(c).wait()
        c_copy(c).wait()
        for i in range(1, O):
            y_copy(i, c).wait_send()
            f_copy(i, c).wait()


def finish_kernel(
    R, units,
    owner_in, tot, master, momentum, sums, bases,
    master_out, momentum_out, params,
    owner, owner_s, ms, mm, su, pb, ps,
    a_s, b_s, u_s, p_s, q_s, oa_s, ob_s, op_s,
):
    blocks = owner.shape[0]
    cols = master.shape[1]
    half = BLOCK_ROWS // 2
    me_s = lax.axis_index("shard")
    get_owner = pltpu.make_async_copy(owner_in, owner, owner_s)
    get_owner.start()

    def unit(shard, place, h):
        if units == 2 * SLOTS:
            return shard * units + 2 * place + h
        moved = shard + jnp.where(place == SLOTS - 1, 1 - 2 * (shard % 2), 0)
        if h:
            moved = moved + jnp.where(moved // 2 == 0, 2, -2)
        return jnp.where(place < 2, shard * units + 2 * place + h, moved * units + units - 1)

    def slot_rows(j):
        return pl.ds(pl.multiple_of(j * BLOCK_ROWS, BLOCK_ROWS), BLOCK_ROWS)

    def get_slot(j):
        return [
            pltpu.make_async_copy(master.at[slot_rows(j)], ms.at[slot_rows(j)], a_s.at[j]),
            pltpu.make_async_copy(momentum.at[slot_rows(j)], mm.at[slot_rows(j)], b_s.at[j]),
        ] + [
            pltpu.make_async_copy(sums.at[unit(me_s, j, h)], su.at[2 * j + h], u_s.at[2 * j + h]) for h in range(2)
        ]

    def put_slot(j):
        return [
            pltpu.make_async_copy(ms.at[slot_rows(j)], master_out.at[slot_rows(j)], oa_s.at[j]),
            pltpu.make_async_copy(mm.at[slot_rows(j)], momentum_out.at[slot_rows(j)], ob_s.at[j]),
        ]

    def get_block(b):
        shard = owner[b, 0]
        place = sum(jnp.where(jnp.logical_and(owner[k, 0] == shard, k < b), 1, 0) for k in range(blocks))
        return [pltpu.make_async_copy(bases.at[shard * SLOTS + place], pb.at[b], p_s.at[b])] + [
            pltpu.make_async_copy(sums.at[unit(shard, place, h)], ps.at[2 * b + h], q_s.at[2 * b + h])
            for h in range(2)
        ]

    def put_block(b):
        return pltpu.make_async_copy(pb.at[b], params.at[slot_rows(b)], op_s.at[b])

    @pl.loop(0, SLOTS)
    def _(j):
        for copy in get_slot(j):
            copy.start()

    get_owner.wait()
    count = shard_count(owner, me_s)

    @pl.loop(0, blocks)
    def _(b):
        for copy in get_block(b):
            copy.start()

    total = jnp.sum(jnp.sum(tot[...], axis=1, keepdims=True), axis=0, keepdims=True)
    limit = 0.5 * jnp.sqrt(jnp.full((1, 1), blocks * BLOCK_ROWS * R * cols, F32))
    factor = jnp.minimum(1.0, limit / (jnp.sqrt(total) + 1e-06))

    @pl.loop(0, SLOTS)
    def _(j):
        for copy in get_slot(j):
            copy.wait()

        @pl.when(j < count)
        def _():
            for h in range(2):
                @pl.loop(0, half // 16)
                def _(r):
                    at = pl.ds(pl.multiple_of(j * BLOCK_ROWS + h * half + r * 16, 16), 16)
                    grad = factor * su[2 * j + h, pl.ds(pl.multiple_of(r * 16, 16), 16), :].astype(F32)
                    fresh = 0.9 * mm[at, :] + grad
                    mm[at, :] = fresh
                    ms[at, :] = ms[at, :] - 0.7 * (grad + 0.9 * fresh)

        for copy in put_slot(j):
            copy.start()

    @pl.loop(0, blocks)
    def _(b):
        for copy in get_block(b):
            copy.wait()
        for h in range(2):
            @pl.loop(0, half // 16)
            def _(r):
                at = pl.ds(pl.multiple_of(h * half + r * 16, 16), 16)
                grad = factor * ps[2 * b + h, pl.ds(pl.multiple_of(r * 16, 16), 16), :].astype(F32)
                pb[b, at, :] = (pb[b, at, :].astype(F32) - 1.33 * grad).astype(BF16)

        put_block(b).start()

    @pl.loop(0, SLOTS)
    def _(j):
        for copy in put_slot(j):
            copy.wait()

    @pl.loop(0, blocks)
    def _(b):
        put_block(b).wait()


def on_device(deltas, master, momentum, block_owner):
    R, S = lax.axis_size("replica"), lax.axis_size("shard")
    width, cols = deltas.shape[2], master.shape[1]
    blocks = block_owner.shape[0]
    half = BLOCK_ROWS // 2
    quad = S == 4 and blocks - SLOTS - (S - 2) <= 2
    rows = 2 * BLOCK_ROWS + half if quad else SLOTS * BLOCK_ROWS
    rc = half
    while rc > 16 and (rows // (rc // 2)) * R <= 160:
        rc //= 2
    chunks = rows // rc
    units = rows // half
    Z, O = R // 2, S // 2
    loads = rows // BLOCK_ROWS + (1 if quad else 0)

    dma = pltpu.SemaphoreType.DMA
    vmem = pltpu.VMEM
    anywhere = pl.BlockSpec(memory_space=pl.ANY)
    in_vmem = pl.BlockSpec(memory_space=pltpu.VMEM)
    in_smem = pl.BlockSpec(memory_space=pltpu.SMEM)
    ys, zs = max(O - 1, 1), max(Z - 1, 1)
    sums, bases, tot = pl.pallas_call(
        functools.partial(sync_kernel, R, S, rows, rc),
        out_shape=(
            jax.ShapeDtypeStruct((S, chunks, rc, cols), BF16),
            jax.ShapeDtypeStruct((S,) + master.shape, BF16),
            jax.ShapeDtypeStruct((8, 128), F32),
        ),
        in_specs=[in_vmem, anywhere, anywhere, anywhere],
        out_specs=(anywhere, anywhere, in_vmem),
        scratch_shapes=[
            vmem((loads * BLOCK_ROWS, width), BF16),
            vmem((BLOCK_ROWS, width) if quad else (16, 128), BF16),
            vmem((half, width) if quad else (16, 128), BF16),
            vmem(master.shape, F32),
            vmem(master.shape, F32),
            vmem(master.shape, BF16),
            vmem((chunks, Z, rc, cols), BF16),
            vmem((chunks, Z, rc, cols), BF16),
            vmem((chunks, zs, rc, cols), BF16),
            vmem((chunks, rc, cols), BF16),
            vmem((2, 8, 128), F32),
            vmem((R - 1, 8, 128), F32),
            vmem((S - 1, 8, 128), F32),
            dma((loads,)), dma((2,)), dma((2,)), dma((2,)), dma, dma,
            dma((chunks, Z)), dma((chunks, Z)),
            dma((chunks, zs)), dma((chunks, zs)),
            dma((chunks,)), dma((chunks,)), dma((chunks,)),
            dma((ys, chunks)), dma((ys, chunks)), dma((ys, chunks)), dma((ys, chunks)),
            dma, dma, dma,
            dma((ys,)), dma((ys,)), dma((ys,)), dma((ys,)),
            dma((R - 1,)), dma((R - 1,)), dma((S - 1,)), dma((S - 1,)),
        ],
        compiler_params=pltpu.CompilerParams(
            collective_id=0, has_side_effects=True, vmem_limit_bytes=VMEM_LIMIT
        ),
        name="sync",
    )(block_owner, deltas, master, momentum)

    return tuple(pl.pallas_call(
        functools.partial(finish_kernel, R, units),
        out_shape=(
            jax.ShapeDtypeStruct(master.shape, F32),
            jax.ShapeDtypeStruct(master.shape, F32),
            jax.ShapeDtypeStruct((blocks * BLOCK_ROWS, cols), BF16),
        ),
        in_specs=[in_vmem, in_vmem] + [anywhere] * 4,
        out_specs=(anywhere,) * 3,
        scratch_shapes=[
            pltpu.SMEM((blocks, 1), jnp.int32), dma,
            vmem(master.shape, F32),
            vmem(master.shape, F32),
            vmem((2 * SLOTS, half, cols), BF16),
            vmem((blocks, BLOCK_ROWS, cols), BF16),
            vmem((2 * blocks, half, cols), BF16),
            dma((SLOTS,)), dma((SLOTS,)), dma((2 * SLOTS,)), dma((blocks,)), dma((2 * blocks,)),
            dma((SLOTS,)), dma((SLOTS,)), dma((blocks,)),
        ],
        compiler_params=pltpu.CompilerParams(vmem_limit_bytes=VMEM_LIMIT),
        name="finish",
    )(block_owner, tot, master, momentum, sums.reshape(S * units, half, cols),
      bases.reshape(S * SLOTS, BLOCK_ROWS, cols)))


def solution(mesh):
    return jax.shard_map(
        on_device,
        mesh=mesh,
        in_specs=(P("replica", "shard", None), P("shard", "replica"), P("shard", "replica"), P()),
        out_specs=(P("shard", "replica"), P("shard", "replica"), P(None, "replica")),
        check_vma=False,
    )
```
